32 devices in a mesh: rows: 8 (over z, y), groups: 4 (over x, core).
Axes of the slice: x: 2, y: 2, z: 4, core: 2. Of those that a mesh axis runs over, the one named last changes fastest.
Arguments:
- basis: bfloat16 [8, 131072, 128], P(None, ('rows', 'groups')), may hold values from -6 to 6
- image: bfloat16 [8, 131072, 128], P(None, ('rows', 'groups')), may hold values from -6 to 6
- selection: int32 [8, 64], replicated, may hold values from 0 to 127, all different within a row
Outputs:
- rotated: bfloat16 [8, 131072, 128], P(None, ('rows', 'groups'))
The draws below stay inside these ranges and needn't reach their ends.
Inputs may be any that keep to these rules, and one draw needn't show every extreme that they name: Each row of selection names 64 different columns.
All inputs are finite; a program needn't handle non-finite values.
Results may differ from the reference program's by a relative error of at most 0.005.
Values may be sent and summed in bfloat16 or wider, within the bound.
A program may use at most 128 MiB of HBM per device.

```python
import jax
import jax.numpy as jnp
from jax import lax

RECYCLE = 64
COLS = 128
NSYS = 8
ITERS = 3
NROWS = 131072


def levels(own_key, shape, shards, smallest, largest):
    gain = 1.0
    for position, shards_of in shards:
        steps = jax.random.uniform(jax.random.fold_in(jax.random.fold_in(own_key, 6), position), (shards_of,), jnp.float32, smallest / len(shards), largest / len(shards))
        gain = gain * jnp.repeat(jnp.exp(steps), shape[position] // shards_of).reshape((-1,) + (1,) * (len(shape) - 1 - position))
    return gain


def picks_of(rng, rows, amount, top, lift):
    sequence = jax.random.permutation(jax.random.fold_in(rng, 1), amount)
    favour = sequence
    for power in range(3):
        favour = favour * favour // amount
    favour = favour * lift // amount
    chance = jax.random.randint(jax.random.fold_in(rng, 2), (rows, amount), 0, 4096) + favour
    sure = jax.random.permutation(jax.random.fold_in(rng, 3), rows)[jnp.arange(amount) % rows]
    chance = jnp.where(jnp.arange(rows)[:, None] == sure[None, :], 1 << 14, chance)
    merit = chance * amount + jnp.arange(amount)
    return lax.top_k(merit.astype(jnp.int32), top)[1].astype(jnp.int32)


def noise(key, dims, scale, limit, split=(), kind=jnp.bfloat16):
    gain = levels(key, dims, split, -0.22, 0.18) if split else 1.0
    values = jax.random.normal(key, dims, jnp.float32) * scale * gain
    return jnp.minimum(jnp.maximum(values, -limit), limit).astype(kind)


def setup_inputs(seed: int = 0) -> dict:
    streams_of = jax.random.split(jax.random.key(seed), 4)
    basis = noise(streams_of[0], (NSYS, NROWS, COLS), 1.0, 6.0, ((1, 32),))
    image = noise(streams_of[1], (NSYS, NROWS, COLS), 1.0, 6.0, ((1, 32),))
    selection = picks_of(streams_of[2], NSYS, COLS, RECYCLE, 0)
    return dict(basis=basis, image=image, selection=selection)


def small_solve(grams, chosen):
    gram_s, cross, gram_f = (grams[0], grams[1], grams[2])
    width = gram_s.shape[0]
    coeffs = (jnp.arange(width, dtype=jnp.int32)[:, None] == chosen[None, :]).astype(jnp.float32)
    factor = jnp.linalg.cholesky(gram_f)
    for step in range(ITERS):
        moved = jnp.dot(cross.T, coeffs, precision=lax.Precision.HIGHEST)
        halfway = lax.linalg.triangular_solve(factor, moved, left_side=True, lower=True)
        solved = lax.linalg.triangular_solve(factor, halfway, left_side=True, lower=True, transpose_a=True)
        metric = jnp.dot(solved.T, jnp.dot(gram_s, solved, precision=lax.Precision.HIGHEST), precision=lax.Precision.HIGHEST) / NROWS
        lower = jnp.linalg.cholesky(metric)
        coeffs = lax.linalg.triangular_solve(lower, solved, left_side=False, lower=True, transpose_a=True)
    return coeffs

def one_system(items):
    left, right, chosen = items
    gram_s = jnp.dot(left.T.astype(jnp.float32), left.astype(jnp.float32), preferred_element_type=jnp.float32)
    cross = jnp.dot(left.T.astype(jnp.float32), right.astype(jnp.float32), preferred_element_type=jnp.float32)
    gram_f = jnp.dot(right.T.astype(jnp.float32), right.astype(jnp.float32), preferred_element_type=jnp.float32)
    coeffs = small_solve(jnp.stack([gram_s, cross, gram_f]), chosen).astype(jnp.bfloat16)
    first = jnp.dot(left.astype(jnp.float32), coeffs.astype(jnp.float32), preferred_element_type=jnp.float32)
    second = jnp.dot(right.astype(jnp.float32), coeffs.astype(jnp.float32), preferred_element_type=jnp.float32)
    return jnp.concatenate([first, second], axis=1).astype(jnp.bfloat16)

def reference(basis, image, selection):
    return lax.map(one_system, (basis, image, selection))
```

```python
import functools

import jax
import jax.numpy as jnp
from jax import lax
from jax.experimental import pallas as pl
from jax.experimental.pallas import tpu as pltpu
from jax.sharding import PartitionSpec as P

ITERS = 3
MESH = pl.DeviceIdType.MESH
NT = (((1,), (1,)), ((), ()))
TN = (((0,), (0,)), ((), ()))
HIGHEST = lax.Precision.HIGHEST


def exact_dot(a, b, dims=(((1,), (0,)), ((), ()))):
    return lax.dot_general(a, b, dims, precision=HIGHEST, preferred_element_type=jnp.float32)


def gram_of(a, b):
    return lax.dot_general(a, b, TN, preferred_element_type=jnp.float32)


def recip(x, refine):
    r = pl.reciprocal(x, approx=True)
    for _ in range(refine):
        r = r * (2.0 - x * r)
    return r


def row_of(tile, j):
    return jnp.broadcast_to(tile[j : j + 1, :], (8, 128))


def spread(tile, lane):
    return jnp.take_along_axis(tile, jnp.full((8, 128), lane, jnp.int32), axis=1)


def eliminate(cols, rest, refine):
    place = lax.broadcasted_iota(jnp.int32, (8, 128), 0)
    saved = []
    for j in range(0, 8, 2):
        c0, c1 = cols[j], cols[j + 1]
        a, b, d = row_of(c0, j), row_of(c1, j), row_of(c1, j + 1)
        det = a * d - b * b
        inv = recip(det, refine)
        ai, bi, di = a * inv, b * inv, d * inv
        first, second = place == j, place == j + 1

        def advance(v, urgent):
            v0, v1 = row_of(v, j), row_of(v, j + 1)
            if urgent:
                u0, u1 = (d * v0 - b * v1) * inv, (a * v1 - b * v0) * inv
            else:
                u0, u1 = di * v0 - bi * v1, ai * v1 - bi * v0
            new = v - c0 * u0 - c1 * u1
            return jnp.where(first, u0, jnp.where(second, u1, new))

        r0, r1 = row_of(rest, j), row_of(rest, j + 1)
        saved.append((r0, a * r1 - b * r0, a, det))
        for k in range(j + 2, len(cols)):
            cols[k] = advance(cols[k], k < j + 4)
        rest = advance(rest, False)
    return cols[8:], rest, saved


def rooted(saved, keep):
    place = lax.broadcasted_iota(jnp.int32, (8, 128), 0)
    tile = jnp.zeros((8, 128), jnp.float32)
    for q in range(4):
        v0, w1, a, det = saved[q]
        root = lax.rsqrt(a)
        tile = jnp.where(place == 2 * q, v0 * root, tile)
        tile = jnp.where(place == 2 * q + 1, w1 * (root * lax.rsqrt(det)), tile)
    return jnp.where(keep, tile, 0.0)


def less(tile, columns, rows):
    for c, r in zip(columns, rows):
        tile = tile - c * r
    return tile


def inverse_root(gram, refine=1):
    n = gram.shape[0]
    lane = lax.broadcasted_iota(jnp.int32, (8, 128), 1)
    place = lax.broadcasted_iota(jnp.int32, (8, 128), 0)
    tiles = [gram[8 * i : 8 * i + 8] for i in range(n // 8)]
    out = []
    for p in range(n // 16):
        first = 16 * p
        inside = jnp.logical_and(lane >= first, lane < first + 16)
        top, low = tiles[2 * p], tiles[2 * p + 1]
        top_cols = [spread(top, first + k) for k in range(16)]
        low_cols = [spread(low, first + k) for k in range(16)]
        far_cols = [[spread(x, first + k) for k in range(16)] for x in tiles[2 * p + 2 :]]
        top = jnp.where(inside, (lane - first == place).astype(jnp.float32), top)
        low = jnp.where(inside, (lane - first == place + 8).astype(jnp.float32), low)
        right, top, saved = eliminate(top_cols, top, refine)
        out.append(rooted(saved, lane < first + 8))
        rows = [row_of(top, k) for k in range(8)]
        low = less(low, low_cols[:8], rows)
        block = [less(low_cols[8 + k], low_cols[:8], [row_of(right[k], j) for j in range(8)]) for k in range(8)]
        _, low, saved = eliminate(block, low, refine)
        out.append(rooted(saved, lane < first + 16))
        rows = [row_of(low, k) for k in range(8)]
        top = less(top, right, rows)
        rows = [row_of(top, k) for k in range(8)] + rows
        for i, cols in enumerate(far_cols):
            j = 2 * p + 2 + i
            tiles[j] = less(jnp.where(inside, 0.0, tiles[j]), cols, rows)
    return jnp.concatenate(out, axis=0)


def padded(x):
    return jnp.concatenate([x, jnp.zeros_like(x)], axis=0)


def symmetric_pack(gram):
    half = gram.shape[0] // 2
    row = lax.broadcasted_iota(jnp.int32, (half, 2 * half), 0)
    lane = lax.broadcasted_iota(jnp.int32, (half, 2 * half), 1)
    low = pltpu.roll(gram[half:], half, 1)
    diag = jnp.sum(jnp.where(row == lane, low, 0.0), axis=0, keepdims=True)
    return jnp.where(lane < row, low, gram[:half]), jnp.broadcast_to(diag, (8, 2 * half))


def symmetric_unpack(packed):
    half = packed.shape[1] // 2
    mixed, diag = packed[:half], packed[half : half + 1]
    row = lax.broadcasted_iota(jnp.int32, (half, 2 * half), 0)
    lane = lax.broadcasted_iota(jnp.int32, (half, 2 * half), 1)
    turned = jnp.concatenate([mixed, jnp.zeros_like(mixed)], axis=0).T
    top = jnp.where(lane < row, turned[:half], mixed)
    low = jnp.where(lane < row, mixed, jnp.where(lane == row, diag, turned[:half]))
    low = jnp.where(lane < half, turned[half:], pltpu.roll(low, half, 1))
    return jnp.concatenate([top, low], axis=0)


def place_of(nsys, n_rows, n_groups):
    inner = nsys // n_groups
    me_r = lax.axis_index("rows")
    me_g = lax.axis_index("groups")
    return me_r // inner, lax.rem(me_r, inner), me_g // 2, lax.rem(me_g, 2)


def coeff_kernel(
    sizes, total_rows, basis, image, selection, held_w, held_q, out, shared, chosen,
    f_own, f_core, f_plane, f_deep, x_own, x_core, x_plane, x_deep, s_own, s_core, s_plane, s_deep,
    load_w, load_q, core_send, core_recv, plane_send, plane_recv, deep_send, deep_recv, csend, crecv, load_c
):
    n_rows, n_groups = sizes
    nsys, _, width = held_w.shape
    half, inner, n_x = nsys // 2, nsys // n_groups, n_groups // 2
    depth = n_rows // inner
    late = min(2, half - 1)
    me_r = lax.axis_index("rows")
    me_g = lax.axis_index("groups")
    z, y, x, c = place_of(nsys, n_rows, n_groups)
    barrier = pltpu.get_barrier_semaphore()
    peers = n_rows * n_groups
    mine = c * half + x * inner + y
    root = lax.rem((depth - 1) // 2 + lax.rem(c + x + y, 2), depth)
    kinds = ((f_own, f_core, f_plane, f_deep), (x_own, x_core, x_plane, x_deep), (s_own, s_core, s_plane, s_deep))

    def at(t):
        rest = lax.rem(t, half)
        core = lax.rem(c + 1 - t // half, 2)
        along = lax.rem(x + n_x - 1 - rest // inner, n_x)
        return core * half + along * inner + lax.rem(y + inner - 1 - lax.rem(rest, inner), inner)

    def nth_peer(i):
        other = lax.rem(me_r * n_groups + me_g + i, peers)
        return (other // n_groups, lax.rem(other, n_groups))

    def load(source, target, sems, s):
        return pltpu.make_async_copy(source.at[s], target.at[s], sems.at[s])

    def to_core(kind, s):
        own, got = kinds[kind][0], kinds[kind][1]
        spot = lax.rem(s, half)
        return pltpu.make_async_remote_copy(
            src_ref=own.at[s],
            dst_ref=got.at[spot],
            send_sem=core_send.at[kind, spot],
            recv_sem=core_recv.at[kind, spot],
            device_id=(me_r, me_g + 1 - 2 * c),
            device_id_type=MESH,
        )

    def in_plane(kind, rest):
        own, got = kinds[kind][0], kinds[kind][2]
        k = lax.rem(x + n_x - 1 - rest // inner, n_x)
        j = lax.rem(y + inner - 1 - lax.rem(rest, inner), inner)
        return pltpu.make_async_remote_copy(
            src_ref=own.at[c * half + k * inner + j],
            dst_ref=got.at[rest],
            send_sem=plane_send.at[kind, rest],
            recv_sem=plane_recv.at[kind, rest],
            device_id=(z * inner + j, k * 2 + c),
            device_id_type=MESH,
        )

    def to_root(kind):
        own, got = kinds[kind][0], kinds[kind][3]
        spot = lax.rem(z - root + depth, depth) - 1
        return pltpu.make_async_remote_copy(
            src_ref=own.at[mine],
            dst_ref=got.at[spot],
            send_sem=deep_send.at[kind],
            recv_sem=deep_recv.at[kind, spot],
            device_id=(root * inner + y, me_g),
            device_id_type=MESH,
        )

    def from_depth(kind, i):
        own, got = kinds[kind][0], kinds[kind][3]
        return pltpu.make_async_remote_copy(
            src_ref=own.at[mine],
            dst_ref=got.at[i],
            send_sem=deep_send.at[kind],
            recv_sem=deep_recv.at[kind, i],
            device_id=(me_r, me_g),
            device_id_type=MESH,
        )

    def plane_sum(kind):
        own, got = kinds[kind][0], kinds[kind][2]
        total = own[mine]
        for rest in range(half - 1):
            in_plane(kind, rest).wait_recv()
            total = total + got[rest]
        return total

    def root_sum(kind):
        total = plane_sum(kind)
        for i in range(depth - 1):
            from_depth(kind, i).wait_recv()
            total = total + kinds[kind][3][i]
        return total

    def first_load(t, carry):
        load(image, held_q, load_q, at(t)).start()
        return carry

    def second_load(t, carry):
        load(basis, held_w, load_w, at(t)).start()
        return carry

    lax.fori_loop(0, nsys, first_load, 0)
    lax.fori_loop(0, nsys, second_load, 0)
    pltpu.make_async_copy(selection, chosen, load_c.at[0]).start()

    def greet(i, carry):
        pl.semaphore_signal(barrier, inc=1, device_id=nth_peer(i), device_id_type=MESH)
        return carry

    lax.fori_loop(1, peers, greet, 0)

    def first_gram(t, carry):
        s = at(t)
        load(image, held_q, load_q, s).wait()
        right = held_q[s]
        mixed, diag = symmetric_pack(gram_of(right, right))
        f_own[s, 0 : width // 2, :] = mixed
        f_own[s, width // 2 :, :] = diag

        @pl.when(t == late)
        def _():
            pl.semaphore_wait(barrier, peers - 1)
            for u in range(late + 1):
                to_core(0, at(u)).start()

        @pl.when(jnp.logical_and(t > late, t < half))
        def _():
            to_core(0, s).start()

        @pl.when(t >= half)
        def _():
            to_core(0, s).wait_recv()
            f_own[s] += f_core[lax.rem(s, half)]

            @pl.when(t < nsys - 1)
            def _():
                in_plane(0, t - half).start()

        return carry

    lax.fori_loop(0, nsys, first_gram, 0)

    def second_gram(t, carry):
        s = at(t)
        load(basis, held_w, load_w, s).wait()
        left = held_w[s]
        pair = gram_of(left, jnp.concatenate([left, held_q[s]], axis=1))
        mixed, diag = symmetric_pack(pair[:, :width])
        s_own[s, 0 : width // 2, :] = mixed
        s_own[s, width // 2 :, :] = diag
        x_own[s] = pair[:, width:]

        @pl.when(t < half)
        def _():
            to_core(1, s).start()
            to_core(2, s).start()

        @pl.when(t >= half)
        def _():
            to_core(1, s).wait_recv()
            x_own[s] += x_core[lax.rem(s, half)]

            @pl.when(t < nsys - 1)
            def _():
                in_plane(1, t - half).start()

            to_core(2, s).wait_recv()
            s_own[s] += s_core[lax.rem(s, half)]

        return carry

    lax.fori_loop(0, nsys, second_gram, 0)

    for rest in range(half - 1):
        in_plane(2, rest).start()
    pltpu.make_async_copy(selection, chosen, load_c.at[0]).wait()

    @pl.when(z != root)
    def _():
        for kind in range(3):
            kinds[kind][0][mine] = plane_sum(kind)
            to_root(kind).start()
        for kind in range(3):
            to_root(kind).wait_send()

    @pl.when(z == root)
    def _():
        half_inverse = inverse_root(symmetric_unpack(root_sum(0)))
        across = exact_dot(exact_dot(root_sum(1), half_inverse, NT), half_inverse)
        gram_s = symmetric_unpack(root_sum(2))
        both = jnp.concatenate([across, exact_dot(across, gram_s)], axis=1)
        picked = chosen[pl.ds(mine, 1), :]
        row = lax.broadcasted_iota(jnp.int32, (width, picked.shape[1]), 0)
        now = exact_dot((row == picked).astype(jnp.float32).T, both)
        for step in range(ITERS):
            solved = now[:, :width]
            last = step == ITERS - 1
            weighted = exact_dot(solved, gram_s) if last else now[:, width:]
            metric = exact_dot(solved, padded(weighted), NT) * (1.0 / total_rows)
            lower = inverse_root(metric, 1 if last else 0)
            now = exact_dot(lower, padded(solved if last else exact_dot(solved, both)))
        shared[pl.ds(mine, 1)] = now.astype(jnp.bfloat16)[None]

        def share(i):
            return pltpu.make_async_remote_copy(
                src_ref=shared.at[mine],
                dst_ref=shared.at[mine],
                send_sem=csend.at[i],
                recv_sem=crecv.at[mine],
                device_id=nth_peer(i),
                device_id_type=MESH,
            )

        def send(i, carry):
            share(i).start()
            return carry

        def sent(i, carry):
            share(i).wait_send()
            return carry

        lax.fori_loop(1, peers, send, 0)
        lax.fori_loop(1, peers, sent, 0)

    for s in range(nsys):

        @pl.when(jnp.logical_or(z != root, mine != s))
        def _():
            pltpu.make_async_remote_copy(
                src_ref=shared.at[s],
                dst_ref=shared.at[s],
                send_sem=csend.at[0],
                recv_sem=crecv.at[s],
                device_id=(me_r, me_g),
                device_id_type=MESH,
            ).wait_recv()

    for kind in range(3):
        for t in range(half):
            to_core(kind, at(t)).wait_send()
        for rest in range(half - 1):
            in_plane(kind, rest).wait_send()
    out[...] = shared[...]


def rotate_kernel(basis, image, coeffs, out):
    narrow = coeffs[0]
    empty = jnp.zeros_like(narrow)
    upper = jnp.concatenate([narrow, empty], axis=1)
    lower = jnp.concatenate([empty, narrow], axis=1)
    both = jnp.concatenate([basis[0], image[0]], axis=1)
    twice = jnp.concatenate([upper, lower], axis=0)
    turned = lax.dot_general(both, twice, NT, preferred_element_type=jnp.float32)
    out[0] = turned.astype(out.dtype)


def on_device(n_rows, n_groups, basis, image, selection):
    nsys, local, width = basis.shape
    keep = selection.shape[1]
    peers = n_rows * n_groups
    total_rows = local * peers
    half, inner = nsys // 2, nsys // n_groups
    depth = n_rows // inner
    near, far = max(half - 1, 1), max(depth - 1, 1)
    packed = width // 2 + 8
    in_hbm = pl.BlockSpec(memory_space=pltpu.HBM)
    in_vmem = pl.BlockSpec(memory_space=pltpu.VMEM)
    held = jax.ShapeDtypeStruct((nsys, local, width), jnp.bfloat16)
    buffers = [
        pltpu.VMEM((count, tall, width), jnp.float32)
        for tall in (packed, width, packed)
        for count in (nsys, half, near, far)
    ]
    held_w, held_q, coeffs = pl.pallas_call(
        functools.partial(coeff_kernel, (n_rows, n_groups), total_rows),
        in_specs=[in_hbm, in_hbm, in_hbm],
        out_specs=[in_vmem, in_vmem, in_vmem],
        out_shape=[held, held, jax.ShapeDtypeStruct((nsys, keep, width), jnp.bfloat16)],
        scratch_shapes=[
            pltpu.VMEM((nsys, keep, width), jnp.bfloat16),
            pltpu.VMEM((nsys, keep), jnp.int32),
            *buffers,
            pltpu.SemaphoreType.DMA((nsys,)),
            pltpu.SemaphoreType.DMA((nsys,)),
            pltpu.SemaphoreType.DMA((3, half)),
            pltpu.SemaphoreType.DMA((3, half)),
            pltpu.SemaphoreType.DMA((3, near)),
            pltpu.SemaphoreType.DMA((3, near)),
            pltpu.SemaphoreType.DMA((3,)),
            pltpu.SemaphoreType.DMA((3, far)),
            pltpu.SemaphoreType.DMA((peers,)),
            pltpu.SemaphoreType.DMA((nsys,)),
            pltpu.SemaphoreType.DMA((1,)),
        ],
        compiler_params=pltpu.CompilerParams(
            collective_id=0,
            has_side_effects=True,
            vmem_limit_bytes=16 << 20,
        ),
    )(*(pltpu.with_memory_space_constraint(v, pltpu.HBM) for v in (basis, image, selection)))
    whole = pl.BlockSpec((1, local, width), lambda s: (s, 0, 0))
    return pl.pallas_call(
        rotate_kernel,
        grid=(nsys,),
        in_specs=[whole, whole, pl.BlockSpec((1, keep, width), lambda s: (s, 0, 0))],
        out_specs=whole,
        out_shape=jax.ShapeDtypeStruct((nsys, local, width), jnp.bfloat16),
        compiler_params=pltpu.CompilerParams(vmem_limit_bytes=16 << 20),
    )(held_w, held_q, coeffs)


def solution(mesh):
    in_specs = (P(None, ("rows", "groups"), None), P(None, ("rows", "groups"), None), P())
    out_specs = P(None, ("rows", "groups"), None)
    return jax.shard_map(
        functools.partial(on_device, mesh.shape["rows"], mesh.shape["groups"]),
        mesh=mesh,
        in_specs=in_specs,
        out_specs=out_specs,
        check_vma=False,
    )
```

```python
import functools

import jax
import jax.numpy as jnp
from jax import lax
from jax.experimental import pallas as pl
from jax.experimental.pallas import tpu as pltpu
from jax.sharding import PartitionSpec as P

ITERS = 3
BATCH = 4
LATE = 0
AHEAD = 3
MESH = pl.DeviceIdType.MESH
NT = (((1,), (1,)), ((), ()))
TN = (((0,), (0,)), ((), ()))
HIGHEST = lax.Precision.HIGHEST


def exact_dot(a, b, dims=(((1,), (0,)), ((), ()))):
    return lax.dot_general(a, b, dims, precision=HIGHEST, preferred_element_type=jnp.float32)


def gram_of(a, b):
    return lax.dot_general(a, b, TN, preferred_element_type=jnp.float32)


def recip(x, refine):
    r = pl.reciprocal(x, approx=True)
    for _ in range(refine):
        r = r * (2.0 - x * r)
    return r


def row_of(tile, j):
    return jnp.broadcast_to(tile[j : j + 1, :], (8, 128))


def spread(tile, lane):
    return jnp.take_along_axis(tile, jnp.full((8, 128), lane, jnp.int32), axis=1)


def eliminate(cols, rest, refine):
    place = lax.broadcasted_iota(jnp.int32, (8, 128), 0)
    saved = []
    for j in range(0, 8, 2):
        c0, c1 = cols[j], cols[j + 1]
        a, b, d = row_of(c0, j), row_of(c1, j), row_of(c1, j + 1)
        det = a * d - b * b
        inv = recip(det, refine)
        ai, bi, di = a * inv, b * inv, d * inv
        first, second = place == j, place == j + 1

        def advance(v, urgent):
            v0, v1 = row_of(v, j), row_of(v, j + 1)
            if urgent:
                u0, u1 = (d * v0 - b * v1) * inv, (a * v1 - b * v0) * inv
            else:
                u0, u1 = di * v0 - bi * v1, ai * v1 - bi * v0
            new = v - c0 * u0 - c1 * u1
            return jnp.where(first, u0, jnp.where(second, u1, new))

        r0, r1 = row_of(rest, j), row_of(rest, j + 1)
        saved.append((r0, a * r1 - b * r0, a, det))
        for k in range(j + 2, len(cols)):
            cols[k] = advance(cols[k], k < j + 4)
        rest = advance(rest, False)
    return cols[8:], rest, saved


def rooted(saved, keep):
    place = lax.broadcasted_iota(jnp.int32, (8, 128), 0)
    tile = jnp.zeros((8, 128), jnp.float32)
    for q in range(4):
        v0, w1, a, det = saved[q]
        root = lax.rsqrt(a)
        tile = jnp.where(place == 2 * q, v0 * root, tile)
        tile = jnp.where(place == 2 * q + 1, w1 * (root * lax.rsqrt(det)), tile)
    return jnp.where(keep, tile, 0.0)


def less(tile, columns, rows):
    for c, r in zip(columns, rows):
        tile = tile - c * r
    return tile


def inverse_root_tiles(gram, refine=1):
    n = gram.shape[0]
    lane = lax.broadcasted_iota(jnp.int32, (8, 128), 1)
    place = lax.broadcasted_iota(jnp.int32, (8, 128), 0)
    tiles = [gram[8 * i : 8 * i + 8] for i in range(n // 8)]
    for p in range(n // 16):
        first = 16 * p
        inside = jnp.logical_and(lane >= first, lane < first + 16)
        top, low = tiles[2 * p], tiles[2 * p + 1]
        top_cols = [spread(top, first + k) for k in range(16)]
        low_cols = [spread(low, first + k) for k in range(16)]
        far_cols = [[spread(x, first + k) for k in range(16)] for x in tiles[2 * p + 2 :]]
        top = jnp.where(inside, (lane - first == place).astype(jnp.float32), top)
        low = jnp.where(inside, (lane - first == place + 8).astype(jnp.float32), low)
        right, top, saved = eliminate(top_cols, top, refine)
        upper = rooted(saved, lane < first + 8)
        rows = [row_of(top, k) for k in range(8)]
        low = less(low, low_cols[:8], rows)
        block = [less(low_cols[8 + k], low_cols[:8], [row_of(right[k], j) for j in range(8)]) for k in range(8)]
        _, low, saved = eliminate(block, low, refine)
        yield upper, rooted(saved, lane < first + 16)
        rows = [row_of(low, k) for k in range(8)]
        top = less(top, right, rows)
        rows = [row_of(top, k) for k in range(8)] + rows
        for i, cols in enumerate(far_cols):
            j = 2 * p + 2 + i
            tiles[j] = less(jnp.where(inside, 0.0, tiles[j]), cols, rows)


def inverse_root(gram, refine=1):
    return jnp.concatenate([x for pair in inverse_root_tiles(gram, refine) for x in pair], axis=0)


def padded(x):
    return jnp.concatenate([x, jnp.zeros_like(x)], axis=0)


def symmetric_pack(gram):
    half = gram.shape[0] // 2
    row = lax.broadcasted_iota(jnp.int32, (half, 2 * half), 0)
    lane = lax.broadcasted_iota(jnp.int32, (half, 2 * half), 1)
    low = pltpu.roll(gram[half:], half, 1)
    diag = jnp.sum(jnp.where(row == lane, low, 0.0), axis=0, keepdims=True)
    return jnp.where(lane < row, low, gram[:half]), jnp.broadcast_to(diag, (8, 2 * half))


def diagonal_row(gram):
    row = lax.broadcasted_iota(jnp.int32, gram.shape, 0)
    lane = lax.broadcasted_iota(jnp.int32, gram.shape, 1)
    diag = jnp.sum(jnp.where(row == lane, gram, 0.0), axis=0, keepdims=True)
    return jnp.broadcast_to(diag, (8, gram.shape[1]))


def symmetric_unpack(packed):
    half = packed.shape[1] // 2
    mixed, diag = packed[:half], packed[half : half + 1]
    row = lax.broadcasted_iota(jnp.int32, (half, 2 * half), 0)
    lane = lax.broadcasted_iota(jnp.int32, (half, 2 * half), 1)
    turned = jnp.concatenate([mixed, jnp.zeros_like(mixed)], axis=0).T
    top = jnp.where(lane < row, turned[:half], mixed)
    low = jnp.where(lane < row, mixed, jnp.where(lane == row, diag, turned[:half]))
    low = jnp.where(lane < half, turned[half:], pltpu.roll(low, half, 1))
    return jnp.concatenate([top, low], axis=0)


def place_of(nsys, n_rows, n_groups):
    inner = nsys // n_groups
    me_r = lax.axis_index("rows")
    me_g = lax.axis_index("groups")
    return me_r // inner, lax.rem(me_r, inner), me_g // 2, lax.rem(me_g, 2)


def coeff_kernel(
    sizes, total_rows, basis, image, selection, held_w, held_q, out, shared, chosen,
    f_own, f_core, f_plane, f_deep, x_top, x_top_core, x_top_plane, x_top_deep,
    x_low, x_low_core, x_low_plane, x_low_deep, s_own, s_core, s_plane, s_deep,
    load_w, load_q, core_send, core_recv, plane_send, plane_recv, deep_send, deep_recv, csend, crecv, load_c
):
    n_rows, n_groups = sizes
    nsys, _, width = held_w.shape
    half, inner, n_x = nsys // 2, nsys // n_groups, n_groups // 2
    depth = n_rows // inner
    batch = BATCH if half % BATCH == 0 else 1
    groups = nsys // batch
    late = min(LATE, groups // 2 - 1)
    me_r = lax.axis_index("rows")
    me_g = lax.axis_index("groups")
    z, y, x, c = place_of(nsys, n_rows, n_groups)
    barrier = pltpu.get_barrier_semaphore()
    peers = n_rows * n_groups
    mine = c * half + x * inner + y
    root = lax.rem((depth - 1) // 2 + lax.rem(c + x + y, 2), depth)
    kinds = (
        (f_own, f_core, f_plane, f_deep),
        (x_top, x_top_core, x_top_plane, x_top_deep),
        (x_low, x_low_core, x_low_plane, x_low_deep),
        (s_own, s_core, s_plane, s_deep),
    )

    def at(t):
        rest = lax.rem(t, half)
        core = lax.rem(c + 1 - t // half, 2)
        along = lax.rem(x + n_x - 1 - rest // inner, n_x)
        return core * half + along * inner + lax.rem(y + inner - 1 - lax.rem(rest, inner), inner)

    def nth_peer(i):
        other = lax.rem(me_r * n_groups + me_g + i, peers)
        return (other // n_groups, lax.rem(other, n_groups))

    def load(source, target, sems, s):
        return pltpu.make_async_copy(source.at[s], target.at[s], sems.at[s])

    def to_core(kind, s):
        own, got = kinds[kind][0], kinds[kind][1]
        spot = lax.rem(s, half)
        return pltpu.make_async_remote_copy(
            src_ref=own.at[s],
            dst_ref=got.at[spot],
            send_sem=core_send.at[kind, spot],
            recv_sem=core_recv.at[kind, spot],
            device_id=(me_r, me_g + 1 - 2 * c),
            device_id_type=MESH,
        )

    def in_plane(kind, rest):
        own, got = kinds[kind][0], kinds[kind][2]
        k = lax.rem(x + n_x - 1 - rest // inner, n_x)
        j = lax.rem(y + inner - 1 - lax.rem(rest, inner), inner)
        return pltpu.make_async_remote_copy(
            src_ref=own.at[c * half + k * inner + j],
            dst_ref=got.at[rest],
            send_sem=plane_send.at[kind, rest],
            recv_sem=plane_recv.at[kind, rest],
            device_id=(z * inner + j, k * 2 + c),
            device_id_type=MESH,
        )

    def to_root(kind):
        own, got = kinds[kind][0], kinds[kind][3]
        spot = lax.rem(z - root + depth, depth) - 1
        return pltpu.make_async_remote_copy(
            src_ref=own.at[mine],
            dst_ref=got.at[spot],
            send_sem=deep_send.at[kind],
            recv_sem=deep_recv.at[kind, spot],
            device_id=(root * inner + y, me_g),
            device_id_type=MESH,
        )

    def from_depth(kind, i):
        own, got = kinds[kind][0], kinds[kind][3]
        return pltpu.make_async_remote_copy(
            src_ref=own.at[mine],
            dst_ref=got.at[i],
            send_sem=deep_send.at[kind],
            recv_sem=deep_recv.at[kind, i],
            device_id=(me_r, me_g),
            device_id_type=MESH,
        )

    def arrived(s):
        return pltpu.make_async_remote_copy(
            src_ref=shared.at[s],
            dst_ref=shared.at[s],
            send_sem=csend.at[0],
            recv_sem=crecv.at[s],
            device_id=(me_r, me_g),
            device_id_type=MESH,
        )

    def plane_sum(kind):
        own, got = kinds[kind][0], kinds[kind][2]
        total = own[mine]
        for rest in range(half - 1):
            in_plane(kind, rest).wait_recv()
            total = total + got[rest]
        return total

    def root_sum(kind):
        total = plane_sum(kind)
        for i in range(depth - 1):
            from_depth(kind, i).wait_recv()
            total = total + kinds[kind][3][i]
        return total

    def start_load(g):
        for u in range(batch):
            if g < groups:
                load(image, held_q, load_q, at(g * batch + u)).start()
            else:
                load(basis, held_w, load_w, at((g - groups) * batch + u)).start()

    for g in range(AHEAD):
        start_load(g)
    pltpu.make_async_copy(selection, chosen, load_c.at[0]).start()

    def greet(i, carry):
        pl.semaphore_signal(barrier, inc=1, device_id=nth_peer(i), device_id_type=MESH)
        return carry

    lax.fori_loop(1, peers, greet, 0)

    def issue(g):
        if g + AHEAD < 2 * groups:
            start_load(g + AHEAD)

    def first_gram(g):
        spots = [at(g * batch + u) for u in range(batch)]
        pieces = [spots[:2], spots[2:]] if g == 0 else [spots]
        for piece in pieces:
            for s in piece:
                load(image, held_q, load_q, s).wait()
            if piece is pieces[-1]:
                issue(g)
            for s in piece:
                right = held_q[s]
                mixed, diag = symmetric_pack(gram_of(right, right))
                f_own[s, 0 : width // 2, :] = mixed
                f_own[s, width // 2 :, :] = diag
        if g == late:
            pl.semaphore_wait(barrier, peers - 1)
            for t in range((late + 1) * batch):
                to_core(0, at(t)).start()
        elif late < g < groups // 2:
            for s in spots:
                to_core(0, s).start()
        if g >= groups // 2:
            for u, s in enumerate(spots):
                to_core(0, s).wait_recv()
                f_own[s] += f_core[lax.rem(s, half)]
                if g * batch + u < nsys - 1:
                    in_plane(0, g * batch + u - half).start()

    def second_gram(g):
        spots = [at(g * batch + u) for u in range(batch)]
        for s in spots:
            load(basis, held_w, load_w, s).wait()
        issue(g + groups)
        for s in spots:
            left = held_w[s]
            pair = gram_of(left, jnp.concatenate([left, held_q[s]], axis=1))
            mixed, diag = symmetric_pack(pair[:, :width])
            s_own[s, 0 : width // 2, :] = mixed
            s_own[s, width // 2 :, :] = diag
            x_top[s] = pair[: width // 2, width:]
            x_low[s, 0 : width // 2, :] = pair[width // 2 :, width:]
            x_low[s, width // 2 :, :] = diagonal_row(pair[:, :width])
        if g < groups // 2:
            for s in spots:
                for kind in (1, 2, 3):
                    to_core(kind, s).start()
        else:
            for kind in (1, 2):
                for u, s in enumerate(spots):
                    own, got = kinds[kind][0], kinds[kind][1]
                    to_core(kind, s).wait_recv()
                    own[s] += got[lax.rem(s, half)]
                    if g * batch + u < nsys - 1:
                        in_plane(kind, g * batch + u - half).start()
            for u, s in enumerate(spots):
                to_core(3, s).wait_recv()
                s_own[s] += s_core[lax.rem(s, half)]
                if g * batch + u < nsys - 1:
                    in_plane(3, g * batch + u - half).start()

    for g in range(groups):
        first_gram(g)
    for g in range(groups):
        second_gram(g)
    pltpu.make_async_copy(selection, chosen, load_c.at[0]).wait()

    @pl.when(z != root)
    def _():
        for kind in range(4):
            kinds[kind][0][mine] = plane_sum(kind)
            to_root(kind).start()
        for kind in range(4):
            to_root(kind).wait_send()

    @pl.when(z == root)
    def _():
        half_inverse = inverse_root(symmetric_unpack(root_sum(0)))
        inverse = exact_dot(half_inverse, half_inverse, TN)
        low = root_sum(2)
        across = exact_dot(jnp.concatenate([root_sum(1), low[: width // 2]], axis=0), inverse)
        weight = jnp.broadcast_to(low[width // 2 : width // 2 + 1], (selection.shape[1], width))
        picked = chosen[pl.ds(mine, 1), :]
        row = lax.broadcasted_iota(jnp.int32, (width, picked.shape[1]), 0)
        solved = exact_dot((row == picked).astype(jnp.float32).T, across)
        for step in range(ITERS - 1):
            metric = exact_dot(solved, padded(solved * weight), NT)
            solved = exact_dot(inverse_root(metric, 0), padded(exact_dot(solved, across)))
        gram_s = symmetric_unpack(root_sum(3))
        metric = exact_dot(solved, padded(exact_dot(solved, gram_s)), NT) * (1.0 / total_rows)
        now = exact_dot(inverse_root(metric), padded(solved))
        shared[pl.ds(mine, 1)] = now.astype(jnp.bfloat16)[None]

        def share(i, far, dx, dy, dc):
            to_row = lax.rem(z + far, depth) * inner + lax.rem(y + dy, inner)
            return pltpu.make_async_remote_copy(
                src_ref=shared.at[mine],
                dst_ref=shared.at[mine],
                send_sem=csend.at[i],
                recv_sem=crecv.at[mine],
                device_id=(to_row, lax.rem(x + dx, n_x) * 2 + lax.rem(c + dc, 2)),
                device_id_type=MESH,
            )

        def steps(o, n):
            return min(o, n - o)

        spots = [
            (far, dx, dy, dc)
            for far in range(depth)
            for dx in range(n_x)
            for dy in range(inner)
            for dc in range(2)
        ][1:]
        spots.sort(key=lambda v: -(steps(v[0], depth) + steps(v[1], n_x) + steps(v[2], inner)))

        for i, spot in enumerate(spots):
            share(i, *spot).start()
        for i, spot in enumerate(spots):
            share(i, *spot).wait_send()

    for s in range(nsys):

        @pl.when(jnp.logical_or(z != root, mine != s))
        def _():
            arrived(s).wait_recv()

    for kind in range(4):
        for t in range(half):
            to_core(kind, at(t)).wait_send()
        for rest in range(half - 1):
            in_plane(kind, rest).wait_send()
    out[...] = shared[...]


def rotate_kernel(basis, image, coeffs, out, ready, sems):
    def store(s):
        return pltpu.make_async_copy(ready.at[s], out.at[s], sems.at[s])

    nsys = basis.shape[0]
    for s in range(nsys):
        narrow = coeffs[s]
        left = lax.dot_general(basis[s], narrow, NT, preferred_element_type=jnp.float32)
        right = lax.dot_general(image[s], narrow, NT, preferred_element_type=jnp.float32)
        ready[s] = jnp.concatenate([left, right], axis=1).astype(out.dtype)
        store(s).start()
    for s in range(nsys):
        store(s).wait()


def on_device(n_rows, n_groups, basis, image, selection):
    nsys, local, width = basis.shape
    keep = selection.shape[1]
    peers = n_rows * n_groups
    total_rows = local * peers
    half, inner = nsys // 2, nsys // n_groups
    depth = n_rows // inner
    near, far = max(half - 1, 1), max(depth - 1, 1)
    packed = width // 2 + 8
    in_hbm = pl.BlockSpec(memory_space=pltpu.HBM)
    in_vmem = pl.BlockSpec(memory_space=pltpu.VMEM)
    held = jax.ShapeDtypeStruct((nsys, local, width), jnp.bfloat16)
    buffers = [
        pltpu.VMEM((count, tall, width), jnp.float32)
        for tall in (packed, width // 2, packed, packed)
        for count in (nsys, half, near, far)
    ]
    held_w, held_q, coeffs = pl.pallas_call(
        functools.partial(coeff_kernel, (n_rows, n_groups), total_rows),
        in_specs=[in_hbm, in_hbm, in_hbm],
        out_specs=[in_vmem, in_vmem, in_vmem],
        out_shape=[held, held, jax.ShapeDtypeStruct((nsys, keep, width), jnp.bfloat16)],
        scratch_shapes=[
            pltpu.VMEM((nsys, keep, width), jnp.bfloat16),
            pltpu.VMEM((nsys, keep), jnp.int32),
            *buffers,
            pltpu.SemaphoreType.DMA((nsys,)),
            pltpu.SemaphoreType.DMA((nsys,)),
            pltpu.SemaphoreType.DMA((4, half)),
            pltpu.SemaphoreType.DMA((4, half)),
            pltpu.SemaphoreType.DMA((4, near)),
            pltpu.SemaphoreType.DMA((4, near)),
            pltpu.SemaphoreType.DMA((4,)),
            pltpu.SemaphoreType.DMA((4, far)),
            pltpu.SemaphoreType.DMA((peers,)),
            pltpu.SemaphoreType.DMA((nsys,)),
            pltpu.SemaphoreType.DMA((1,)),
        ],
        compiler_params=pltpu.CompilerParams(
            collective_id=0,
            has_side_effects=True,
            vmem_limit_bytes=16 << 20,
        ),
    )(*(pltpu.with_memory_space_constraint(v, pltpu.HBM) for v in (basis, image, selection)))
    return pl.pallas_call(
        rotate_kernel,
        in_specs=[in_vmem, in_vmem, in_vmem],
        out_specs=in_hbm,
        out_shape=held,
        scratch_shapes=[pltpu.VMEM((nsys, local, width), jnp.bfloat16), pltpu.SemaphoreType.DMA((nsys,))],
        compiler_params=pltpu.CompilerParams(vmem_limit_bytes=16 << 20),
    )(held_w, held_q, coeffs)


def solution(mesh):
    in_specs = (P(None, ("rows", "groups"), None), P(None, ("rows", "groups"), None), P())
    out_specs = P(None, ("rows", "groups"), None)
    return jax.shard_map(
        functools.partial(on_device, mesh.shape["rows"], mesh.shape["groups"]),
        mesh=mesh,
        in_specs=in_specs,
        out_specs=out_specs,
        check_vma=False,
    )
```

```python
import functools

import jax
import jax.numpy as jnp
from jax import lax
from jax.experimental import pallas as pl
from jax.experimental.pallas import tpu as pltpu
from jax.sharding import PartitionSpec as P

ITERS = 3
BATCH = 4
LATE = 0
AHEAD = 3
MESH = pl.DeviceIdType.MESH
NT = (((1,), (1,)), ((), ()))
TN = (((0,), (0,)), ((), ()))
HIGHEST = lax.Precision.HIGHEST


def exact_dot(a, b, dims=(((1,), (0,)), ((), ()))):
    return lax.dot_general(a, b, dims, precision=HIGHEST, preferred_element_type=jnp.float32)


def gram_of(a, b):
    return lax.dot_general(a, b, TN, preferred_element_type=jnp.float32)


def recip(x, refine):
    r = pl.reciprocal(x, approx=True)
    for _ in range(refine):
        r = r * (2.0 - x * r)
    return r


def row_of(tile, j):
    return jnp.broadcast_to(tile[j : j + 1, :], (8, 128))


def spread(tile, lane):
    return jnp.take_along_axis(tile, jnp.full((8, 128), lane, jnp.int32), axis=1)


def eliminate(cols, rest, refine):
    place = lax.broadcasted_iota(jnp.int32, (8, 128), 0)
    saved = []
    for j in range(0, 8, 2):
        c0, c1 = cols[j], cols[j + 1]
        a, b, d = row_of(c0, j), row_of(c1, j), row_of(c1, j + 1)
        det = a * d - b * b
        inv = recip(det, refine)
        ai, bi, di = a * inv, b * inv, d * inv
        first, second = place == j, place == j + 1

        def advance(v, urgent):
            v0, v1 = row_of(v, j), row_of(v, j + 1)
            if urgent:
                u0, u1 = (d * v0 - b * v1) * inv, (a * v1 - b * v0) * inv
            else:
                u0, u1 = di * v0 - bi * v1, ai * v1 - bi * v0
            new = v - c0 * u0 - c1 * u1
            return jnp.where(first, u0, jnp.where(second, u1, new))

        r0, r1 = row_of(rest, j), row_of(rest, j + 1)
        saved.append((r0, a * r1 - b * r0, a, det))
        for k in range(j + 2, len(cols)):
            cols[k] = advance(cols[k], k < j + 4)
        rest = advance(rest, False)
    return cols[8:], rest, saved


def rooted(saved, keep):
    place = lax.broadcasted_iota(jnp.int32, (8, 128), 0)
    tile = jnp.zeros((8, 128), jnp.float32)
    for q in range(4):
        v0, w1, a, det = saved[q]
        root = lax.rsqrt(a)
        tile = jnp.where(place == 2 * q, v0 * root, tile)
        tile = jnp.where(place == 2 * q + 1, w1 * (root * lax.rsqrt(det)), tile)
    return jnp.where(keep, tile, 0.0)


def less(tile, columns, rows):
    for c, r in zip(columns, rows):
        tile = tile - c * r
    return tile


def inverse_root_tiles(gram, refine=1):
    n = gram.shape[0]
    lane = lax.broadcasted_iota(jnp.int32, (8, 128), 1)
    place = lax.broadcasted_iota(jnp.int32, (8, 128), 0)
    tiles = [gram[8 * i : 8 * i + 8] for i in range(n // 8)]
    for p in range(n // 16):
        first = 16 * p
        inside = jnp.logical_and(lane >= first, lane < first + 16)
        top, low = tiles[2 * p], tiles[2 * p + 1]
        top_cols = [spread(top, first + k) for k in range(16)]
        low_cols = [spread(low, first + k) for k in range(16)]
        far_cols = [[spread(x, first + k) for k in range(16)] for x in tiles[2 * p + 2 :]]
        top = jnp.where(inside, (lane - first == place).astype(jnp.float32), top)
        low = jnp.where(inside, (lane - first == place + 8).astype(jnp.float32), low)
        right, top, saved = eliminate(top_cols, top, refine)
        upper = rooted(saved, lane < first + 8)
        rows = [row_of(top, k) for k in range(8)]
        low = less(low, low_cols[:8], rows)
        block = [less(low_cols[8 + k], low_cols[:8], [row_of(right[k], j) for j in range(8)]) for k in range(8)]
        _, low, saved = eliminate(block, low, refine)
        yield upper, rooted(saved, lane < first + 16)
        rows = [row_of(low, k) for k in range(8)]
        top = less(top, right, rows)
        rows = [row_of(top, k) for k in range(8)] + rows
        for i, cols in enumerate(far_cols):
            j = 2 * p + 2 + i
            tiles[j] = less(jnp.where(inside, 0.0, tiles[j]), cols, rows)


def inverse_root(gram, refine=1):
    return jnp.concatenate([x for pair in inverse_root_tiles(gram, refine) for x in pair], axis=0)


def padded(x):
    return jnp.concatenate([x, jnp.zeros_like(x)], axis=0)


def symmetric_pack(gram):
    half = gram.shape[0] // 2
    row = lax.broadcasted_iota(jnp.int32, (half, 2 * half), 0)
    lane = lax.broadcasted_iota(jnp.int32, (half, 2 * half), 1)
    low = pltpu.roll(gram[half:], half, 1)
    diag = jnp.sum(jnp.where(row == lane, low, 0.0), axis=0, keepdims=True)
    return jnp.where(lane < row, low, gram[:half]), jnp.broadcast_to(diag, (8, 2 * half))


def diagonal_row(gram):
    row = lax.broadcasted_iota(jnp.int32, gram.shape, 0)
    lane = lax.broadcasted_iota(jnp.int32, gram.shape, 1)
    diag = jnp.sum(jnp.where(row == lane, gram, 0.0), axis=0, keepdims=True)
    return jnp.broadcast_to(diag, (8, gram.shape[1]))


def symmetric_unpack(packed):
    half = packed.shape[1] // 2
    mixed, diag = packed[:half], packed[half : half + 1]
    row = lax.broadcasted_iota(jnp.int32, (half, 2 * half), 0)
    lane = lax.broadcasted_iota(jnp.int32, (half, 2 * half), 1)
    turned = jnp.concatenate([mixed, jnp.zeros_like(mixed)], axis=0).T
    top = jnp.where(lane < row, turned[:half], mixed)
    low = jnp.where(lane < row, mixed, jnp.where(lane == row, diag, turned[:half]))
    low = jnp.where(lane < half, turned[half:], pltpu.roll(low, half, 1))
    return jnp.concatenate([top, low], axis=0)


def place_of(nsys, n_rows, n_groups):
    inner = nsys // n_groups
    me_r = lax.axis_index("rows")
    me_g = lax.axis_index("groups")
    return me_r // inner, lax.rem(me_r, inner), me_g // 2, lax.rem(me_g, 2)


def coeff_kernel(
    sizes, total_rows, basis, image, selection, held_w, held_q, out, shared, chosen, raw,
    f_own, f_core, f_plane, f_deep, x_top, x_top_core, x_top_plane, x_top_deep,
    x_low, x_low_core, x_low_plane, x_low_deep, s_own, s_core, s_plane, s_deep,
    load_w, load_q, core_send, core_recv, plane_send, plane_recv, deep_send, deep_recv, csend, crecv, load_c
):
    n_rows, n_groups = sizes
    nsys, _, width = held_w.shape
    half, inner, n_x = nsys // 2, nsys // n_groups, n_groups // 2
    depth = n_rows // inner
    batch = BATCH if half % BATCH == 0 else 1
    groups = nsys // batch
    late = min(LATE, groups // 2 - 1)
    me_r = lax.axis_index("rows")
    me_g = lax.axis_index("groups")
    z, y, x, c = place_of(nsys, n_rows, n_groups)
    barrier = pltpu.get_barrier_semaphore()
    peers = n_rows * n_groups
    mine = c * half + x * inner + y
    root = lax.rem((depth - 1) // 2 + lax.rem(c + x + y, 2), depth)
    kinds = (
        (f_own, f_core, f_plane, f_deep),
        (x_top, x_top_core, x_top_plane, x_top_deep),
        (x_low, x_low_core, x_low_plane, x_low_deep),
        (s_own, s_core, s_plane, s_deep),
    )

    def at(t):
        rest = lax.rem(t, half)
        core = lax.rem(c + 1 - t // half, 2)
        along = lax.rem(x + n_x - 1 - rest // inner, n_x)
        return core * half + along * inner + lax.rem(y + inner - 1 - lax.rem(rest, inner), inner)

    def nth_peer(i):
        other = lax.rem(me_r * n_groups + me_g + i, peers)
        return (other // n_groups, lax.rem(other, n_groups))

    def load(source, target, sems, s):
        return pltpu.make_async_copy(source.at[s], target.at[s], sems.at[s])

    def to_core(kind, s):
        own, got = kinds[kind][0], kinds[kind][1]
        spot = lax.rem(s, half)
        return pltpu.make_async_remote_copy(
            src_ref=own.at[s],
            dst_ref=got.at[spot],
            send_sem=core_send.at[kind, spot],
            recv_sem=core_recv.at[kind, spot],
            device_id=(me_r, me_g + 1 - 2 * c),
            device_id_type=MESH,
        )

    def in_plane(kind, rest):
        own, got = kinds[kind][0], kinds[kind][2]
        k = lax.rem(x + n_x - 1 - rest // inner, n_x)
        j = lax.rem(y + inner - 1 - lax.rem(rest, inner), inner)
        return pltpu.make_async_remote_copy(
            src_ref=own.at[c * half + k * inner + j],
            dst_ref=got.at[rest],
            send_sem=plane_send.at[kind, rest],
            recv_sem=plane_recv.at[kind, rest],
            device_id=(z * inner + j, k * 2 + c),
            device_id_type=MESH,
        )

    def to_root(kind):
        own, got = kinds[kind][0], kinds[kind][3]
        spot = lax.rem(z - root + depth, depth) - 1
        return pltpu.make_async_remote_copy(
            src_ref=own.at[mine],
            dst_ref=got.at[spot],
            send_sem=deep_send.at[kind],
            recv_sem=deep_recv.at[kind, spot],
            device_id=(root * inner + y, me_g),
            device_id_type=MESH,
        )

    def from_depth(kind, i):
        own, got = kinds[kind][0], kinds[kind][3]
        return pltpu.make_async_remote_copy(
            src_ref=own.at[mine],
            dst_ref=got.at[i],
            send_sem=deep_send.at[kind],
            recv_sem=deep_recv.at[kind, i],
            device_id=(me_r, me_g),
            device_id_type=MESH,
        )

    def arrived(s):
        return pltpu.make_async_remote_copy(
            src_ref=shared.at[s],
            dst_ref=shared.at[s],
            send_sem=csend.at[0],
            recv_sem=crecv.at[s],
            device_id=(me_r, me_g),
            device_id_type=MESH,
        )

    def plane_sum(kind):
        own, got = kinds[kind][0], kinds[kind][2]
        total = own[mine]
        for rest in range(half - 1):
            in_plane(kind, rest).wait_recv()
            total = total + got[rest]
        return total

    def root_sum(kind):
        total = plane_sum(kind)
        for i in range(depth - 1):
            from_depth(kind, i).wait_recv()
            total = total + kinds[kind][3][i]
        return total

    def start_load(g):
        for u in range(batch):
            if g < groups:
                load(image, held_q, load_q, at(g * batch + u)).start()
            else:
                load(basis, held_w, load_w, at((g - groups) * batch + u)).start()

    for g in range(AHEAD):
        start_load(g)
    pltpu.make_async_copy(selection, chosen, load_c.at[0]).start()

    def greet(i, carry):
        pl.semaphore_signal(barrier, inc=1, device_id=nth_peer(i), device_id_type=MESH)
        return carry

    lax.fori_loop(1, peers, greet, 0)

    def issue(g):
        if g + AHEAD < 2 * groups:
            start_load(g + AHEAD)

    def first_gram(g):
        spots = [at(g * batch + u) for u in range(batch)]
        pieces = [spots[:2], spots[2:]] if g == 0 else [spots]
        for piece in pieces:
            for s in piece:
                load(image, held_q, load_q, s).wait()
            if piece is pieces[-1]:
                issue(g)
            for s in piece:
                right = held_q[s]
                mixed, diag = symmetric_pack(gram_of(right, right))
                f_own[s, 0 : width // 2, :] = mixed
                f_own[s, width // 2 :, :] = diag
        if g == late:
            pl.semaphore_wait(barrier, peers - 1)
            for t in range((late + 1) * batch):
                to_core(0, at(t)).start()
        elif late < g < groups // 2:
            for s in spots:
                to_core(0, s).start()
        if g >= groups // 2:
            for u, s in enumerate(spots):
                to_core(0, s).wait_recv()
                f_own[s] += f_core[lax.rem(s, half)]
                if g * batch + u < nsys - 1:
                    in_plane(0, g * batch + u - half).start()

    def pack_s(spots):
        for u, s in enumerate(spots):
            mixed, diag = symmetric_pack(raw[u])
            s_own[s, 0 : width // 2, :] = mixed
            s_own[s, width // 2 :, :] = diag

    def second_gram(g):
        spots = [at(g * batch + u) for u in range(batch)]
        for s in spots:
            load(basis, held_w, load_w, s).wait()
        issue(g + groups)
        for u, s in enumerate(spots):
            left = held_w[s]
            pair = gram_of(left, jnp.concatenate([left, held_q[s]], axis=1))
            raw[u] = pair[:, :width]
            x_top[s] = pair[: width // 2, width:]
            x_low[s, 0 : width // 2, :] = pair[width // 2 :, width:]
            x_low[s, width // 2 :, :] = diagonal_row(pair[:, :width])
        if g < groups // 2:
            for s in spots:
                for kind in (1, 2):
                    to_core(kind, s).start()
            pack_s(spots)
            for s in spots:
                to_core(3, s).start()
        else:
            for kind in (1, 2):
                for u, s in enumerate(spots):
                    own, got = kinds[kind][0], kinds[kind][1]
                    to_core(kind, s).wait_recv()
                    own[s] += got[lax.rem(s, half)]
                    if g * batch + u < nsys - 1:
                        in_plane(kind, g * batch + u - half).start()
            pack_s(spots)
            for u, s in enumerate(spots):
                to_core(3, s).wait_recv()
                s_own[s] += s_core[lax.rem(s, half)]
                if g * batch + u < nsys - 1:
                    in_plane(3, g * batch + u - half).start()

    for g in range(groups):
        first_gram(g)
    for g in range(groups):
        second_gram(g)
    pltpu.make_async_copy(selection, chosen, load_c.at[0]).wait()

    @pl.when(z != root)
    def _():
        for kind in range(4):
            kinds[kind][0][mine] = plane_sum(kind)
            to_root(kind).start()
        for kind in range(4):
            to_root(kind).wait_send()

    @pl.when(z == root)
    def _():
        half_inverse = inverse_root(symmetric_unpack(root_sum(0)))
        inverse = exact_dot(half_inverse, half_inverse, TN)
        low = root_sum(2)
        across = exact_dot(jnp.concatenate([root_sum(1), low[: width // 2]], axis=0), inverse)
        weight = jnp.broadcast_to(low[width // 2 : width // 2 + 1], (selection.shape[1], width))
        picked = chosen[pl.ds(mine, 1), :]
        row = lax.broadcasted_iota(jnp.int32, (width, picked.shape[1]), 0)
        solved = exact_dot((row == picked).astype(jnp.float32).T, across)
        for step in range(ITERS - 1):
            metric = exact_dot(solved, padded(solved * weight), NT)
            solved = exact_dot(inverse_root(metric, 0), padded(exact_dot(solved, across)))
        gram_s = symmetric_unpack(root_sum(3))
        metric = exact_dot(solved, padded(exact_dot(solved, gram_s)), NT) * (1.0 / total_rows)
        now = exact_dot(inverse_root(metric), padded(solved))
        shared[pl.ds(mine, 1)] = now.astype(jnp.bfloat16)[None]

        def share(i, far, dx, dy, dc):
            to_row = lax.rem(z + far, depth) * inner + lax.rem(y + dy, inner)
            return pltpu.make_async_remote_copy(
                src_ref=shared.at[mine],
                dst_ref=shared.at[mine],
                send_sem=csend.at[i],
                recv_sem=crecv.at[mine],
                device_id=(to_row, lax.rem(x + dx, n_x) * 2 + lax.rem(c + dc, 2)),
                device_id_type=MESH,
            )

        def steps(o, n):
            return min(o, n - o)

        spots = [
            (far, dx, dy, dc)
            for far in range(depth)
            for dx in range(n_x)
            for dy in range(inner)
            for dc in range(2)
        ][1:]
        spots.sort(key=lambda v: -(steps(v[0], depth) + steps(v[1], n_x) + steps(v[2], inner)))

        for i, spot in enumerate(spots):
            share(i, *spot).start()
        for i, spot in enumerate(spots):
            share(i, *spot).wait_send()

    for s in range(nsys):

        @pl.when(jnp.logical_or(z != root, mine != s))
        def _():
            arrived(s).wait_recv()

    for kind in range(4):
        for t in range(half):
            to_core(kind, at(t)).wait_send()
        for rest in range(half - 1):
            in_plane(kind, rest).wait_send()
    out[...] = shared[...]


def rotate_kernel(basis, image, coeffs, out, ready, sems):
    def store(s):
        return pltpu.make_async_copy(ready.at[s], out.at[s], sems.at[s])

    nsys = basis.shape[0]
    for s in range(nsys):
        narrow = coeffs[s]
        left = lax.dot_general(basis[s], narrow, NT, preferred_element_type=jnp.float32)
        right = lax.dot_general(image[s], narrow, NT, preferred_element_type=jnp.float32)
        ready[s] = jnp.concatenate([left, right], axis=1).astype(out.dtype)
        store(s).start()
    for s in range(nsys):
        store(s).wait()


def on_device(n_rows, n_groups, basis, image, selection):
    nsys, local, width = basis.shape
    keep = selection.shape[1]
    peers = n_rows * n_groups
    total_rows = local * peers
    half, inner = nsys // 2, nsys // n_groups
    depth = n_rows // inner
    near, far = max(half - 1, 1), max(depth - 1, 1)
    packed = width // 2 + 8
    in_hbm = pl.BlockSpec(memory_space=pltpu.HBM)
    in_vmem = pl.BlockSpec(memory_space=pltpu.VMEM)
    held = jax.ShapeDtypeStruct((nsys, local, width), jnp.bfloat16)
    buffers = [
        pltpu.VMEM((count, tall, width), jnp.float32)
        for tall in (packed, width // 2, packed, packed)
        for count in (nsys, half, near, far)
    ]
    held_w, held_q, coeffs = pl.pallas_call(
        functools.partial(coeff_kernel, (n_rows, n_groups), total_rows),
        in_specs=[in_hbm, in_hbm, in_hbm],
        out_specs=[in_vmem, in_vmem, in_vmem],
        out_shape=[held, held, jax.ShapeDtypeStruct((nsys, keep, width), jnp.bfloat16)],
        scratch_shapes=[
            pltpu.VMEM((nsys, keep, width), jnp.bfloat16),
            pltpu.VMEM((nsys, keep), jnp.int32),
            pltpu.VMEM((max(BATCH, 1), width, width), jnp.float32),
            *buffers,
            pltpu.SemaphoreType.DMA((nsys,)),
            pltpu.SemaphoreType.DMA((nsys,)),
            pltpu.SemaphoreType.DMA((4, half)),
            pltpu.SemaphoreType.DMA((4, half)),
            pltpu.SemaphoreType.DMA((4, near)),
            pltpu.SemaphoreType.DMA((4, near)),
            pltpu.SemaphoreType.DMA((4,)),
            pltpu.SemaphoreType.DMA((4, far)),
            pltpu.SemaphoreType.DMA((peers,)),
            pltpu.SemaphoreType.DMA((nsys,)),
            pltpu.SemaphoreType.DMA((1,)),
        ],
        compiler_params=pltpu.CompilerParams(
            collective_id=0,
            has_side_effects=True,
            vmem_limit_bytes=16 << 20,
        ),
    )(*(pltpu.with_memory_space_constraint(v, pltpu.HBM) for v in (basis, image, selection)))
    return pl.pallas_call(
        rotate_kernel,
        in_specs=[in_vmem, in_vmem, in_vmem],
        out_specs=in_hbm,
        out_shape=held,
        scratch_shapes=[pltpu.VMEM((nsys, local, width), jnp.bfloat16), pltpu.SemaphoreType.DMA((nsys,))],
        compiler_params=pltpu.CompilerParams(vmem_limit_bytes=16 << 20),
    )(held_w, held_q, coeffs)


def solution(mesh):
    in_specs = (P(None, ("rows", "groups"), None), P(None, ("rows", "groups"), None), P())
    out_specs = P(None, ("rows", "groups"), None)
    return jax.shard_map(
        functools.partial(on_device, mesh.shape["rows"], mesh.shape["groups"]),
        mesh=mesh,
        in_specs=in_specs,
        out_specs=out_specs,
        check_vma=False,
    )
```
